128 devices in a mesh: rep: 1, r: 4 (over x), s: 32 (over y, z, core).
Axes of the slice: x: 4, y: 4, z: 4, core: 2. Of those that a mesh axis runs over, the one named last changes fastest.
Arguments:
- x: bfloat16 [128, 2048, 1280], P(('rep', 'r', 's'))
- dy: bfloat16 [128, 2048, 1280], P(('rep', 'r', 's'))
- w_gate: bfloat16 [2, 1280, 3584], P(None, 's')
- w_up: bfloat16 [2, 1280, 3584], P(None, 's')
- w_down: bfloat16 [2, 3584, 1280], P(None, 's')
- m_w_gate: float32 [2, 1280, 3584], P(None, 's')
- m_w_up: float32 [2, 1280, 3584], P(None, 's')
- m_w_down: float32 [2, 3584, 1280], P(None, 's')
- v_w_gate: float32 [2, 1280, 3584], P(None, 's')
- v_w_up: float32 [2, 1280, 3584], P(None, 's')
- v_w_down: float32 [2, 3584, 1280], P(None, 's')
Outputs:
- output 1: bfloat16 [2, 1280, 3584], P('rep', 's')
- output 2: bfloat16 [2, 1280, 3584], P('rep', 's')
- output 3: bfloat16 [2, 3584, 1280], P('rep', 's')
- output 4: float32 [2, 1280, 3584], P('rep', 's')
- output 5: float32 [2, 1280, 3584], P('rep', 's')
- output 6: float32 [2, 3584, 1280], P('rep', 's')
- output 7: float32 [2, 1280, 3584], P('rep', 's')
- output 8: float32 [2, 1280, 3584], P('rep', 's')
- output 9: float32 [2, 3584, 1280], P('rep', 's')
All inputs are finite; a program needn't handle non-finite values.
Results may differ from the reference program's by a relative error of at most 0.022.
Values are sent between devices in bfloat16 or wider.
A program may use at most 1.5 GiB of HBM per device.

```python
import jax
import jax.numpy as jnp
from jax import lax

SEQUENCES = 128
TOKENS = 2048
D = 1280
FF = 3584
LAYERS = 2
NAMES = ("w_gate", "w_up", "w_down")
SHAPES = {"w_gate": (LAYERS, D, FF), "w_up": (LAYERS, D, FF), "w_down": (LAYERS, FF, D)}


def bump(key, n, height):
    away = (jnp.arange(n, dtype=jnp.int32) - jax.random.randint(key, (), 0, n, jnp.int32)) % n
    return jnp.where(away < n // 8, height, 1.0)


def together(key, own, strength):
    shared = jax.random.normal(key, own.shape[1:], jnp.float32)
    return (own + strength * shared) * lax.rsqrt(1 + strength * strength)


def setup_inputs(seed: int = 0, part: int = 0) -> dict:
    kx, kdy, ka, kb, kz, kf, kh, kl, *keys = jax.random.split(jax.random.key(seed), 8 + 3 * len(NAMES))
    kx, kdy, ka, kb = (jax.random.fold_in(k, part) for k in (kx, kdy, ka, kb))
    kw, km, kv = (keys[i::3] for i in range(3))
    shape = (SEQUENCES, TOKENS, D)
    much_x, much_dy = jax.random.uniform(kz, (2,), jnp.float32, 0.0, 1.0)
    loud = 2.0 ** jax.random.uniform(jax.random.fold_in(kz, 1), (), jnp.float32, -1.0, 2.0)
    layers = 2.0 ** jax.random.uniform(kl, (LAYERS, 1, 1), jnp.float32, -1.0, 1.0)
    x = together(ka, jax.random.normal(kx, shape, jnp.float32), much_x) * bump(kf, D, 4.0)
    dy = together(kb, jax.random.normal(kdy, shape, jnp.float32), much_dy)
    drawn = {"x": x.astype(jnp.bfloat16), "dy": (loud * dy * (SEQUENCES * TOKENS) ** -0.5).astype(jnp.bfloat16)}
    for key, name in zip(kw, NAMES, strict=True):
        w = jax.random.normal(key, SHAPES[name], jnp.float32) * SHAPES[name][1] ** -0.5
        drawn[name] = (w * {"w_gate": 1.0, "w_up": bump(kh, FF, 4.0), "w_down": layers}[name]).astype(jnp.bfloat16)
    for key, name in zip(km, NAMES, strict=True):
        drawn[f"m_{name}"] = 0.1 * jax.random.normal(key, SHAPES[name], jnp.float32)
    for key, name in zip(kv, NAMES, strict=True):
        drawn[f"v_{name}"] = jax.random.uniform(key, SHAPES[name], jnp.float32, 0.005, 0.015)
    return drawn


def matmul(a, w):
    return jnp.dot(a, w, preferred_element_type=jnp.float32).astype(jnp.bfloat16)


def normed(h):
    wide = h.astype(jnp.float32)
    scale = lax.rsqrt(jnp.mean(wide**2, -1, keepdims=True) + 1e-6)
    return (wide * scale).astype(jnp.bfloat16)


def layer(h, w):
    a = normed(h)
    gate = jnp.dot(a, w["w_gate"], preferred_element_type=jnp.float32)
    up = jnp.dot(a, w["w_up"], preferred_element_type=jnp.float32)
    return h + matmul((jax.nn.silu(gate) * up).astype(jnp.bfloat16), w["w_down"])


def adamw(w, m, v, g):
    m = 0.9 * m + 0.1 * g
    v = 0.95 * v + 0.05 * g * g
    step = m * lax.rsqrt(v + 1e-8) + 0.1 * w
    return (w - 0.02 * step).astype(jnp.bfloat16), m, v


def clipped(gradients, sum_of_squares, count):
    factor = jnp.minimum(1.0, 0.5 * lax.rsqrt(sum_of_squares / count + 1e-30))
    return [g * factor for g in gradients]


def stack(weights, h):
    return lax.scan(lambda h, w: (layer(h, w), None), h, weights)[0]


def reference(x, dy, w_gate, w_up, w_down, m_w_gate, m_w_up, m_w_down, v_w_gate, v_w_up, v_w_down):
    weights = dict(zip(NAMES, (w_gate, w_up, w_down), strict=True))

    def take(so_far, sequence):
        h, by_y = sequence
        _, back = jax.vjp(lambda w: stack(w, h), weights)
        return jax.tree.map(lambda total, term: total + term.astype(jnp.float32), so_far, back(by_y)[0]), None

    none_yet = {name: jnp.zeros(w.shape, jnp.float32) for name, w in weights.items()}
    by_weights, _ = lax.scan(take, none_yet, (x, dy))
    gradients = [by_weights[name].astype(jnp.bfloat16).astype(jnp.float32) for name in NAMES]
    gradients = clipped(gradients, sum(jnp.sum(g * g) for g in gradients), sum(g.size for g in gradients))
    new = [
        adamw(w.astype(jnp.float32), m, v, g)
        for w, m, v, g in zip((w_gate, w_up, w_down), (m_w_gate, m_w_up, m_w_down), (v_w_gate, v_w_up, v_w_down), gradients, strict=True)
    ]
    return tuple(one[which] for which in range(3) for one in new)
```

```python
import jax
import jax.numpy as jnp
from jax import lax
from jax.sharding import Mesh
from jax.sharding import PartitionSpec as P

F32, BF16 = jnp.float32, jnp.bfloat16
SWAP = [(0, 1), (1, 0)]


def dot(a, b, ca=1, cb=0):
    return lax.dot_general(a, b, (((ca,), (cb,)), ((), ())), preferred_element_type=F32)


def normed(h):
    wide = h.astype(F32)
    scale = lax.rsqrt(jnp.mean(wide**2, -1, keepdims=True) + 1e-6)
    return (wide * scale).astype(BF16)


def adamw(w, m, v, g):
    m = 0.9 * m + 0.1 * g
    v = 0.95 * v + 0.05 * g * g
    step = m * lax.rsqrt(v + 1e-8) + 0.1 * w
    return (w - 0.02 * step).astype(BF16), m, v


def solution(mesh):
    reps, groups, shards = (mesh.shape[a] for a in ("rep", "r", "s"))
    chips = shards // 2
    fine = Mesh(mesh.devices.reshape(reps, groups, chips, 2), ("rep", "r", "q", "c"))
    to_half = [(s, 2 * (s % chips) + s // chips) for s in range(shards)]
    from_half = [(b, a) for a, b in to_half]
    near = [(i, i ^ 1) for i in range(groups)]
    wrap = [(i, groups - 1 - i) for i in range(groups)]

    def step(x, dy, *arrays):
        weights, m, v = (arrays[i : i + 3] for i in (0, 3, 6))
        layers = weights[0].shape[0]
        first = lax.axis_index("c") == 0

        def columns(w):
            low, high = jnp.split(w, 2, axis=-1)
            keep, send = jnp.where(first, low, high), jnp.where(first, high, low)
            came = lax.ppermute(send, "c", SWAP)
            return jnp.concatenate([jnp.where(first, keep, came), jnp.where(first, came, keep)], 0)

        def fetched(name, number):
            w = weights[name][number]
            part = lax.ppermute(w, ("q", "c"), to_half) if name == 2 else columns(w)
            mine = lax.all_gather(part, "q", axis=0, tiled=True)
            return mine, lax.ppermute(mine, "c", SWAP)

        def summed(name, mine, other):
            half = (mine + lax.ppermute(other, "c", SWAP).astype(F32)).astype(BF16)
            part = lax.psum_scatter(half, "q", scatter_dimension=0, tiled=True)
            if name == 2:
                block = lax.ppermute(part, ("q", "c"), from_half)
            else:
                low, high = jnp.split(part, 2, axis=0)
                keep, send = jnp.where(first, low, high), jnp.where(first, high, low)
                came = lax.ppermute(send, "c", SWAP)
                block = jnp.concatenate([jnp.where(first, keep, came), jnp.where(first, came, keep)], 1)
            pieces = []
            for piece, ways in zip(jnp.split(block, 2, axis=1), ((near, wrap), (wrap, near)), strict=True):
                for way in ways:
                    piece = (piece.astype(F32) + lax.ppermute(piece, "r", way).astype(F32)).astype(BF16)
                pieces.append(piece)
            return jnp.concatenate(pieces, 1)

        full = [[fetched(name, number) for name in range(3)] for number in range(layers)]
        h, kept = x[0], []
        for number in range(layers):
            a, back = jax.vjp(normed, h)
            gates = [dot(a, w) for w in full[number][0]]
            ups = [dot(a, w) for w in full[number][1]]
            acts = [(jax.nn.silu(g) * u).astype(BF16) for g, u in zip(gates, ups, strict=True)]
            kept.append((a, back, gates, ups, acts))
            if number < layers - 1:
                h = h + sum(dot(t, w) for t, w in zip(acts, full[number][2], strict=True)).astype(BF16)

        by_h, blocks = dy[0], [[None] * layers for _ in range(3)]
        for number in reversed(range(layers)):
            a, back, gates, ups, acts = kept[number]
            blocks[2][number] = summed(2, dot(acts[0], by_h, 0, 0), dot(acts[1], by_h, 0, 0).astype(BF16))
            by_gate, by_up = [None] * 2, [None] * 2
            for i in (1, 0):
                by_act = dot(by_h, full[number][2][i], 1, 1).astype(BF16).astype(F32)
                on = jax.nn.sigmoid(gates[i])
                by_up[i] = (by_act * (gates[i] * on)).astype(BF16)
                by_gate[i] = (by_act * ups[i] * (on * (1.0 + gates[i] * (1.0 - on)))).astype(BF16)
            for name, by in ((0, by_gate), (1, by_up)):
                blocks[name][number] = summed(name, dot(a, by[0], 0, 0), dot(a, by[1], 0, 0).astype(BF16))
            if number > 0:
                by_a = [sum(dot(t, w, 1, 1) for t, w in zip(by, full[number][name], strict=True)).astype(BF16) for name, by in ((0, by_gate), (1, by_up))]
                by_h = by_h + back(by_a[0] + by_a[1])[0]

        gradients = [jnp.stack(b).astype(F32) for b in blocks]
        squares = lax.psum(sum(jnp.sum(g * g) for g in gradients), ("r", "q", "c")) / groups
        count = shards * sum(g.size for g in gradients)
        factor = jnp.minimum(1.0, 0.5 * lax.rsqrt(squares / count + 1e-30))
        new = [adamw(w.astype(F32), m, v, g * factor) for w, m, v, g in zip(weights, m, v, gradients, strict=True)]
        return tuple(one[which] for which in range(3) for one in new)

    states, cut = P(("rep", "r", "q", "c"), None, None), P(None, ("q", "c"), None)
    return jax.shard_map(
        step,
        mesh=fine,
        in_specs=(states, states) + (cut,) * 9,
        out_specs=(P("rep", ("q", "c"), None),) * 9,
        check_vma=False,
    )
```

```python
import functools

import jax
import jax.numpy as jnp
from jax import lax
from jax.experimental import pallas as pl
from jax.experimental.pallas import tpu as pltpu
from jax.sharding import Mesh
from jax.sharding import PartitionSpec as P

F32, BF16 = jnp.float32, jnp.bfloat16
MESH = pl.DeviceIdType.MESH
SWAP = [(0, 1), (1, 0)]
NAMES = ("w_gate", "w_up", "w_down")
TILE = 256
SIDE = 4


def matmul(a, w):
    return jnp.dot(a, w, preferred_element_type=F32).astype(BF16)


def normed(h):
    wide = h.astype(F32)
    scale = lax.rsqrt(jnp.mean(wide**2, -1, keepdims=True) + 1e-6)
    return (wide * scale).astype(BF16)


def adamw(w, m, v, g):
    m = 0.9 * m + 0.1 * g
    v = 0.95 * v + 0.05 * g * g
    step = m * lax.rsqrt(v + 1e-8) + 0.1 * w
    return (w - 0.02 * step).astype(BF16), m, v


def near(x):
    return x + 1 - 2 * lax.rem(x, 2)


def wrap(x):
    return SIDE - 1 - x


def upper(rows):
    return (rows // 16 + 1) // 2 * 16


class Host:
    pass


def gradient_call(number, product=None, scatter=None, across=None):
    operands, in_specs, out_shapes, out_specs, scratch = [], [], [], [], []
    names_in, names_out, names_scratch = [], [], []
    anywhere, vmem = pl.BlockSpec(memory_space=pl.ANY), pl.BlockSpec(memory_space=pltpu.VMEM)
    dma = pltpu.SemaphoreType.DMA

    def take(name, value, spec):
        operands.append(value), in_specs.append(spec), names_in.append(name)

    def give(name, shape, dtype, spec):
        out_shapes.append(jax.ShapeDtypeStruct(shape, dtype)), out_specs.append(spec), names_out.append(name)

    def hold(name, what):
        scratch.append(what), names_scratch.append(name)

    steps, tiles, flops, moved = 1, 0, 0, 0
    if product:
        kind, resident, streamed = product
        tokens, half = streamed.shape[0], streamed.shape[1] // 2
        tiles = half // TILE
        d = resident.shape[0] if kind == "columns" else resident.shape[1]
        tile = (d, TILE) if kind == "columns" else (TILE, d)

        def place(i):
            n = jnp.clip(i - tiles, 0, tiles - 1)
            return (0, n) if kind == "columns" else (n, 0)

        whole = (d, half) if kind == "columns" else (half, d)
        take("resident", resident, vmem)
        take("streamed", streamed, anywhere)
        give("wide", whole, F32, pl.BlockSpec(tile, place))
        give("narrow", whole, BF16, pl.BlockSpec(tile, place))
        hold("stream", pltpu.VMEM((2, tokens, TILE), BF16))
        hold("stream_sem", dma((2,)))
        hold("sent", pltpu.VMEM((tiles, *tile), BF16))
        hold("came", pltpu.VMEM((tiles, *tile), BF16))
        hold("pair_send", dma((tiles,)))
        hold("pair_recv", dma((tiles,)))
        steps = max(steps, 2 * tiles)
        flops += 4 * tokens * half * d
        moved += streamed.size * 2 + resident.size * 2 + 6 * d * half
    if scatter:
        wide, narrow = scatter
        rows, columns = wide.shape[2:]
        part = columns // 2
        cut = upper(rows)
        take("wide_in", wide, anywhere)
        take("narrow_in", narrow, anywhere)
        give("block", (rows, columns), BF16, vmem)
        hold("held", pltpu.VMEM((2, 3, SIDE, rows, part), F32))
        hold("held_sem", dma((2, 3)))
        hold("got1", pltpu.VMEM((2, 2, 2, rows, part), BF16))
        hold("put2", pltpu.VMEM((2, 2, SIDE, rows, part), BF16))
        hold("got2", pltpu.VMEM((2, 2, SIDE, rows, part), BF16))
        hold("put3", pltpu.VMEM((2, rows, part), BF16))
        hold("got3", pltpu.VMEM((2, rows, part), BF16))
        hold("put4", pltpu.VMEM((2, 2, rows, part), BF16))
        hold("got4", pltpu.VMEM((2, 2, rows, part), BF16))
        hold("ring_send", dma((4, 2, 2)))
        hold("ring_recv", dma((4, 2, 2)))
        steps = max(steps, 17)
    if across is not None:
        wide_rows, wide_columns = across.shape
        take("partial", across, vmem)
        give("total", across.shape, BF16, vmem)
        hold("across_got", pltpu.VMEM((2, *across.shape), BF16))
        hold("across_put", pltpu.VMEM(across.shape, BF16))
        hold("across_send", dma((2, 2)))
        hold("across_recv", dma((2, 2)))
        steps = max(steps, 11)

    def kernel(*refs):
        k = Host()
        for name, ref in zip(names_in + names_out + names_scratch, refs, strict=True):
            setattr(k, name, ref)
        i = pl.program_id(0)
        x, q, c = lax.axis_index("r"), lax.axis_index("q"), lax.axis_index("c")
        at = (q // SIDE, lax.rem(q, SIDE))

        def beside(axis, by):
            there = lax.rem(at[axis] + by + SIDE, SIDE)
            return {"q": there * SIDE + at[1] if axis == 0 else at[0] * SIDE + there}

        peers = []
        if product:
            peers.append({"c": 1 - c})
        if scatter:
            peers += [beside(axis, by) for axis in (0, 1) for by in (1, -1)]
        if across is not None:
            peers += [{"r": near(x)}, {"r": wrap(x)}]

        def send(src, dst, send_sem, recv_sem, to):
            return pltpu.make_async_remote_copy(src_ref=src, dst_ref=dst, send_sem=send_sem, recv_sem=recv_sem, device_id=to, device_id_type=MESH)

        events = {}

        def when(step):
            def add(f):
                events.setdefault(step, []).append(f)
                return f

            return add

        @when(0)
        def _():
            barrier = pltpu.get_barrier_semaphore()
            for peer in peers:
                pl.semaphore_signal(barrier, inc=1, device_id=peer, device_id_type=MESH)
            pl.semaphore_wait(barrier, len(peers))

        if scatter:
            spans = (pl.ds(0, part), pl.ds(part, part))

            def places(p, by):
                return lax.rem(at[p] + by + SIDE, SIDE)

            def of(ref, p, by, some):
                return ref.at[places(p, by), some, :, spans[p]] if p == 0 else ref.at[some, places(p, by), :, spans[p]]

            def loads():
                return [
                    pltpu.make_async_copy(of(k.wide_in, p, by, pl.ds(0, SIDE)), k.held.at[p, n], k.held_sem.at[p, n])
                    for p in (0, 1)
                    for n, by in enumerate((0, 1, -1))
                ]

            def ring(stage):
                copies = []
                for p in (0, 1):
                    for n, by in enumerate((1, -1)):
                        if stage == 0:
                            src, dst, axis = of(k.narrow_in, p, 2, pl.ds(2 * n, 2)), k.got1.at[p, n], p
                        elif stage == 1:
                            src, dst, axis = k.put2.at[p, n], k.got2.at[p, n], p
                        elif stage == 2:
                            some = pl.ds(0, cut) if n == 0 else pl.ds(cut, rows - cut)
                            src, dst, axis = k.put3.at[p, some], k.got3.at[p, some], 1 - p
                        else:
                            src, dst, axis = k.put4.at[p, n], k.got4.at[p, n], 1 - p
                        copies.append(send(src, dst, k.ring_send.at[stage, p, n], k.ring_recv.at[stage, p, n], beside(axis, by)))
                return copies

            @when(0)
            def _():
                for copy in ring(0) + loads():
                    copy.start()

            @when(4)
            def _():
                for copy in ring(0) + loads():
                    copy.wait()
                for p in (0, 1):
                    for n in (0, 1):
                        for s in range(SIDE):
                            value = k.held[p, n + 1, s]
                            if s // 2 == n:
                                value = value + k.got1[p, n, s % 2].astype(F32)
                            k.put2[p, n, s] = value.astype(BF16)

            @when(5)
            def _():
                for copy in ring(1):
                    copy.start()

            @when(12)
            def _():
                for copy in ring(1):
                    copy.wait()
                for p in (0, 1):
                    for s in range(SIDE):
                        k.held[p, 0, s] = k.held[p, 0, s] + k.got2[p, 0, s].astype(F32) + k.got2[p, 1, s].astype(F32)
                    k.put3[p] = k.held[p, 0, places(1 - p, 2)].astype(BF16)

            @when(13)
            def _():
                for copy in ring(2):
                    copy.start()

            @when(14)
            def _():
                for copy in ring(2):
                    copy.wait()
                for p in (0, 1):
                    ahead, behind = places(1 - p, 1), places(1 - p, -1)
                    k.put4[p, 0, :cut] = (k.held[p, 0, ahead, :cut] + k.got3[p, :cut].astype(F32)).astype(BF16)
                    k.put4[p, 0, cut:] = k.held[p, 0, ahead, cut:].astype(BF16)
                    k.put4[p, 1, :cut] = k.held[p, 0, behind, :cut].astype(BF16)
                    k.put4[p, 1, cut:] = (k.held[p, 0, behind, cut:] + k.got3[p, cut:].astype(F32)).astype(BF16)

            @when(15)
            def _():
                for copy in ring(3):
                    copy.start()

            @when(16)
            def _():
                for copy in ring(3):
                    copy.wait()
                for p in (0, 1):
                    mine = k.held[p, 0, places(1 - p, 0)]
                    k.block[:, p * part : (p + 1) * part] = (mine + k.got4[p, 0].astype(F32) + k.got4[p, 1].astype(F32)).astype(BF16)

        if across is not None:
            sides = (pl.ds(0, wide_columns // 2), pl.ds(wide_columns // 2, wide_columns // 2))
            ways = ((near, wrap), (wrap, near))

            def swaps(stage):
                src = k.partial if stage == 0 else k.across_put
                return [
                    send(src.at[:, sides[p]], k.across_got.at[stage, :, sides[p]], k.across_send.at[stage, p], k.across_recv.at[stage, p], {"r": ways[p][stage](x)})
                    for p in (0, 1)
                ]

            @when(0)
            def _():
                for copy in swaps(0):
                    copy.start()

            @when(4)
            def _():
                for copy in swaps(0):
                    copy.wait()
                k.across_put[...] = (k.partial[...].astype(F32) + k.across_got[0].astype(F32)).astype(BF16)

            @when(5)
            def _():
                for copy in swaps(1):
                    copy.start()

            @when(10)
            def _():
                for copy in swaps(1):
                    copy.wait()
                k.total[...] = (k.across_put[...].astype(F32) + k.across_got[1].astype(F32)).astype(BF16)

        if product:

            def fetch(n):
                theirs = (n < tiles).astype(jnp.int32)
                which = theirs * (1 - c) + (1 - theirs) * c
                column = pl.multiple_of(which * half + (n - tiles * (1 - theirs)) * TILE, TILE)
                slot = lax.rem(n, 2)
                return pltpu.make_async_copy(k.streamed.at[:, pl.ds(column, TILE)], k.stream.at[slot], k.stream_sem.at[slot])

            def to_partner(n):
                return send(k.sent.at[n], k.came.at[n], k.pair_send.at[n], k.pair_recv.at[n], {"c": 1 - c})

            @when(0)
            def _():
                fetch(i).start()

        for step in sorted(events):

            @pl.when(i == step)
            def _(step=step):
                for f in events[step]:
                    f()

        if product:

            @pl.when(jnp.logical_and(i >= 1, i <= tiles))
            def _():
                to_partner(i - 1).start()

            @pl.when(i < 2 * tiles)
            def _():
                fetch(i).wait()

                @pl.when(i + 1 < 2 * tiles)
                def _():
                    fetch(i + 1).start()

                block = k.stream[lax.rem(i, 2)]
                if kind == "columns":
                    value = jnp.dot(k.resident[...], block, preferred_element_type=F32)
                else:
                    value = lax.dot_general(block, k.resident[...], (((0,), (0,)), ((), ())), preferred_element_type=F32)

                @pl.when(i < tiles)
                def _():
                    k.sent[i] = value.astype(BF16)

                @pl.when(i >= tiles)
                def _():
                    to_partner(i - tiles).wait()
                    both = value + k.came[i - tiles].astype(F32)
                    k.wide[...] = both
                    k.narrow[...] = both.astype(BF16)

    call = pl.pallas_call(
        kernel,
        grid=(steps,),
        out_shape=out_shapes,
        in_specs=in_specs,
        out_specs=out_specs,
        scratch_shapes=scratch,
        compiler_params=pltpu.CompilerParams(
            collective_id=number, has_side_effects=True, dimension_semantics=("arbitrary",), vmem_limit_bytes=62 * 1024 * 1024
        ),
        cost_estimate=pl.CostEstimate(flops=max(flops, 10**9), bytes_accessed=max(moved, 10**6), transcendentals=0),
        name=f"gradient{number}",
    )
    return dict(zip(names_out, call(*operands), strict=True))


def plane_sum(number, value, chips):
    count = 2 * chips

    def kernel(value_ref, total_ref, got, send_sem, recv_sem):
        q, c = lax.axis_index("q"), lax.axis_index("c")
        me = 2 * q + c
        barrier = pltpu.get_barrier_semaphore()
        peers = [lax.rem(me + n, count) for n in range(1, count)]
        for peer in peers:
            pl.semaphore_signal(barrier, inc=1, device_id={"q": peer // 2, "c": lax.rem(peer, 2)}, device_id_type=MESH)
        pl.semaphore_wait(barrier, count - 1)
        copies = [
            pltpu.make_async_remote_copy(
                src_ref=value_ref,
                dst_ref=got.at[n],
                send_sem=send_sem.at[n],
                recv_sem=recv_sem.at[n],
                device_id={"q": peer // 2, "c": lax.rem(peer, 2)},
                device_id_type=MESH,
            )
            for n, peer in enumerate(peers)
        ]
        for copy in copies:
            copy.start()
        for copy in copies:
            copy.wait()
        total = value_ref[...]
        for n in range(count - 1):
            total = total + got[n]
        total_ref[...] = total

    return pl.pallas_call(
        kernel,
        out_shape=jax.ShapeDtypeStruct((8, 128), F32),
        in_specs=[pl.BlockSpec(memory_space=pltpu.VMEM)],
        out_specs=pl.BlockSpec(memory_space=pltpu.VMEM),
        scratch_shapes=[pltpu.VMEM((count - 1, 8, 128), F32), pltpu.SemaphoreType.DMA((count - 1,)), pltpu.SemaphoreType.DMA((count - 1,))],
        compiler_params=pltpu.CompilerParams(collective_id=number, has_side_effects=True),
        name="plane_sum",
    )(jnp.full((8, 128), value, F32))[0, 0]


def solution(mesh):
    reps, groups, shards = (mesh.shape[a] for a in ("rep", "r", "s"))
    chips = shards // 2
    fine = Mesh(mesh.devices.reshape(reps, groups, chips, 2), ("rep", "r", "q", "c"))
    from_half = [(2 * (s % chips) + s // chips, s) for s in range(shards)]

    def step(x, dy, *arrays):
        weights, m, v = (arrays[i : i + 3] for i in (0, 3, 6))
        layers = weights[0].shape[0]
        first = lax.axis_index("c") == 0

        def own(name, total):
            if name == 2:
                return lax.ppermute(total, ("q", "c"), from_half)
            low, high = jnp.split(total, 2, axis=0)
            keep, send = jnp.where(first, low, high), jnp.where(first, high, low)
            came = lax.ppermute(send, "c", SWAP)
            return jnp.concatenate([jnp.where(first, keep, came), jnp.where(first, came, keep)], 1)

        full = [[lax.all_gather(w[number], ("q", "c"), axis=0, tiled=True) for w in weights] for number in range(layers)]
        h, kept = x[0], []
        for number in range(layers):
            w = full[number]
            a, back = jax.vjp(normed, h)
            gate = jnp.dot(a, w[0], preferred_element_type=F32)
            up = jnp.dot(a, w[1], preferred_element_type=F32)
            act = (jax.nn.silu(gate) * up).astype(BF16)
            kept.append((a, back, gate, up, act))
            if number < layers - 1:
                h = h + matmul(act, w[2])

        queue, totals = [], [[None] * layers for _ in range(3)]
        state = {"number": 0, "scatter": None, "across": None}

        def run(product=None, name=None, number=None):
            s, t = state["scatter"], state["across"]
            given = gradient_call(state["number"], product, s and s[1], None if t is None else t[1])
            state["number"] += 1
            state["scatter"] = state["across"] = None
            if t is not None:
                totals[t[0][0]][t[0][1]] = given["total"]
            if s is not None:
                state["across"] = (s[0], given["block"])
            if product is not None:
                shape = (SIDE, SIDE, given["wide"].shape[0] // chips, given["wide"].shape[1])
                state["scatter"] = ((name, number), (given["wide"].reshape(shape), given["narrow"].reshape(shape)))

        by_h = dy[0]
        for number in reversed(range(layers)):
            w = full[number]
            a, back, gate, up, act = kept[number]
            across_tokens = a.T
            run(("rows", by_h, act), 2, number)
            by_act = lax.dot_general(by_h, w[2], (((1,), (1,)), ((), ())), preferred_element_type=F32).astype(BF16).astype(F32)
            on = jax.nn.sigmoid(gate)
            by_up = (by_act * (gate * on)).astype(BF16)
            by_gate = (by_act * up * (on * (1.0 + gate * (1.0 - on)))).astype(BF16)
            run(("columns", across_tokens, by_gate), 0, number)
            run(("columns", across_tokens, by_up), 1, number)
            if number > 0:
                by_a = [
                    lax.dot_general(by, w[i], (((1,), (1,)), ((), ())), preferred_element_type=F32).astype(BF16) for i, by in ((0, by_gate), (1, by_up))
                ]
                by_h = by_h + back(by_a[0] + by_a[1])[0]
        run()
        run()

        squares = sum(jnp.sum(t.astype(F32) ** 2) for one in totals for t in one)
        squares = plane_sum(state["number"], squares, chips)
        gradients = [jnp.stack([own(name, t) for t in one]).astype(F32) for name, one in enumerate(totals)]
        count = shards * sum(g.size for g in gradients)
        factor = jnp.minimum(1.0, 0.5 * lax.rsqrt(squares / count + 1e-30))
        new = [adamw(w.astype(F32), m, v, g * factor) for w, m, v, g in zip(weights, m, v, gradients, strict=True)]
        return tuple(one[which] for which in range(3) for one in new)

    states, cut = P(("rep", "r", "q", "c"), None, None), P(None, ("q", "c"), None)
    return jax.shard_map(
        step,
        mesh=fine,
        in_specs=(states, states) + (cut,) * 9,
        out_specs=(P("rep", ("q", "c"), None),) * 9,
        check_vma=False,
    )
```

```python
import functools

import jax
import jax.numpy as jnp
from jax import lax
from jax.experimental import pallas as pl
from jax.experimental.pallas import tpu as pltpu
from jax.sharding import Mesh
from jax.sharding import PartitionSpec as P

F32, BF16 = jnp.float32, jnp.bfloat16
MESH = pl.DeviceIdType.MESH
SWAP = [(0, 1), (1, 0)]
NAMES = ("w_gate", "w_up", "w_down")
TILE = 256
SIDE = 4


def matmul(a, w):
    return jnp.dot(a, w, preferred_element_type=F32).astype(BF16)


def normed(h):
    wide = h.astype(F32)
    scale = lax.rsqrt(jnp.mean(wide**2, -1, keepdims=True) + 1e-6)
    return (wide * scale).astype(BF16)


def adamw(w, m, v, g):
    m = 0.9 * m + 0.1 * g
    v = 0.95 * v + 0.05 * g * g
    step = m * lax.rsqrt(v + 1e-8) + 0.1 * w
    return (w - 0.02 * step).astype(BF16), m, v


def near(x):
    return x + 1 - 2 * lax.rem(x, 2)


def wrap(x):
    return SIDE - 1 - x


def upper(rows):
    return (rows // 16 + 1) // 2 * 16


class Host:
    pass


def gradient_call(number, product=None, scatter=None, finish=None, across=None):
    operands, in_specs, out_shapes, out_specs, scratch = [], [], [], [], []
    names_in, names_out, names_scratch = [], [], []
    anywhere, vmem = pl.BlockSpec(memory_space=pl.ANY), pl.BlockSpec(memory_space=pltpu.VMEM)
    dma = pltpu.SemaphoreType.DMA

    def take(name, value, spec):
        operands.append(value), in_specs.append(spec), names_in.append(name)

    def give(name, shape, dtype, spec):
        out_shapes.append(jax.ShapeDtypeStruct(shape, dtype)), out_specs.append(spec), names_out.append(name)

    def hold(name, what):
        scratch.append(what), names_scratch.append(name)

    steps, tiles, flops, moved = 1, 0, 0, 0
    if product:
        kind, resident, streamed = product
        tokens, half = streamed.shape[0], streamed.shape[1] // 2
        tiles = half // TILE
        d = resident.shape[0] if kind == "columns" else resident.shape[1]
        tile = (d, TILE) if kind == "columns" else (TILE, d)

        def place(i):
            n = jnp.clip(i - tiles, 0, tiles - 1)
            return (0, n) if kind == "columns" else (n, 0)

        whole = (d, half) if kind == "columns" else (half, d)
        take("resident", resident, vmem)
        take("streamed", streamed, anywhere)
        give("wide", whole, F32, pl.BlockSpec(tile, place))
        give("narrow", whole, BF16, pl.BlockSpec(tile, place))
        hold("stream", pltpu.VMEM((2, tokens, TILE), BF16))
        hold("stream_sem", dma((2,)))
        hold("sent", pltpu.VMEM((tiles, *tile), BF16))
        hold("came", pltpu.VMEM((tiles, *tile), BF16))
        hold("pair_send", dma((tiles,)))
        hold("pair_recv", dma((tiles,)))
        steps = max(steps, 2 * tiles)
        flops += 4 * tokens * half * d
        moved += streamed.size * 2 + resident.size * 2 + 6 * d * half
    if scatter:
        wide, narrow = scatter
        rows, columns = wide.shape[2:]
        part = columns // 2
        take("wide_in", wide, anywhere)
        take("narrow_in", narrow, anywhere)
        give("kept", (2, SIDE, rows, part), F32, vmem)
        give("third", (2, rows, part), BF16, vmem)
        hold("held", pltpu.VMEM((2, 3, SIDE, rows, part), F32))
        hold("held_sem", dma((2, 3)))
        hold("got1", pltpu.VMEM((2, 2, 2, rows, part), BF16))
        hold("put2", pltpu.VMEM((2, 2, SIDE, rows, part), BF16))
        hold("got2", pltpu.VMEM((2, 2, SIDE, rows, part), BF16))
        hold("ring_send", dma((2, 2, 2)))
        hold("ring_recv", dma((2, 2, 2)))
        steps = max(steps, 13)
    if finish:
        last_rows, last_part = finish[1].shape[1:]
        cut = upper(last_rows)
        take("kept_in", finish[0], vmem)
        take("third_in", finish[1], vmem)
        give("block", (last_rows, 2 * last_part), BF16, vmem)
        hold("got3", pltpu.VMEM((2, last_rows, last_part), BF16))
        hold("put4", pltpu.VMEM((2, 2, last_rows, last_part), BF16))
        hold("got4", pltpu.VMEM((2, 2, last_rows, last_part), BF16))
        hold("last_send", dma((2, 2, 2)))
        hold("last_recv", dma((2, 2, 2)))
        steps = max(steps, 10)
    if across is not None:
        wide_rows, wide_columns = across.shape
        take("partial", across, vmem)
        give("total", across.shape, BF16, vmem)
        hold("across_got", pltpu.VMEM((2, *across.shape), BF16))
        hold("across_put", pltpu.VMEM(across.shape, BF16))
        hold("across_send", dma((2, 2)))
        hold("across_recv", dma((2, 2)))
        steps = max(steps, 11)

    def kernel(*refs):
        k = Host()
        for name, ref in zip(names_in + names_out + names_scratch, refs, strict=True):
            setattr(k, name, ref)
        i = pl.program_id(0)
        x, q, c = lax.axis_index("r"), lax.axis_index("q"), lax.axis_index("c")
        at = (q // SIDE, lax.rem(q, SIDE))

        def beside(axis, by):
            there = lax.rem(at[axis] + by + SIDE, SIDE)
            return {"q": there * SIDE + at[1] if axis == 0 else at[0] * SIDE + there}

        peers = []
        if product:
            peers.append({"c": 1 - c})
        if scatter or finish:
            peers += [beside(axis, by) for axis in (0, 1) for by in (1, -1)]
        if across is not None:
            peers += [{"r": near(x)}, {"r": wrap(x)}]

        def send(src, dst, send_sem, recv_sem, to):
            return pltpu.make_async_remote_copy(src_ref=src, dst_ref=dst, send_sem=send_sem, recv_sem=recv_sem, device_id=to, device_id_type=MESH)

        events = {}

        def when(step):
            def add(f):
                events.setdefault(step, []).append(f)
                return f

            return add

        @when(0)
        def _():
            barrier = pltpu.get_barrier_semaphore()
            for peer in peers:
                pl.semaphore_signal(barrier, inc=1, device_id=peer, device_id_type=MESH)
            pl.semaphore_wait(barrier, len(peers))

        def places(p, by):
            return lax.rem(at[p] + by + SIDE, SIDE)

        if scatter:
            spans = (pl.ds(0, part), pl.ds(part, part))

            def of(ref, p, by, some):
                return ref.at[places(p, by), some, :, spans[p]] if p == 0 else ref.at[some, places(p, by), :, spans[p]]

            def loads():
                return [
                    pltpu.make_async_copy(of(k.wide_in, p, by, pl.ds(0, SIDE)), k.held.at[p, n], k.held_sem.at[p, n])
                    for p in (0, 1)
                    for n, by in enumerate((0, 1, -1))
                ]

            def ring(stage):
                copies = []
                for p in (0, 1):
                    for n, by in enumerate((1, -1)):
                        if stage == 0:
                            src, dst, axis = of(k.narrow_in, p, 2, pl.ds(2 * n, 2)), k.got1.at[p, n], p
                        else:
                            src, dst, axis = k.put2.at[p, n], k.got2.at[p, n], p
                        copies.append(send(src, dst, k.ring_send.at[stage, p, n], k.ring_recv.at[stage, p, n], beside(axis, by)))
                return copies

            @when(0)
            def _():
                for copy in ring(0) + loads():
                    copy.start()

            @when(4)
            def _():
                for copy in ring(0) + loads():
                    copy.wait()
                for p in (0, 1):
                    for n in (0, 1):
                        for s in range(SIDE):
                            value = k.held[p, n + 1, s]
                            if s // 2 == n:
                                value = value + k.got1[p, n, s % 2].astype(F32)
                            k.put2[p, n, s] = value.astype(BF16)

            @when(5)
            def _():
                for copy in ring(1):
                    copy.start()

            @when(12)
            def _():
                for copy in ring(1):
                    copy.wait()
                for p in (0, 1):
                    for s in range(SIDE):
                        k.kept[p, s] = k.held[p, 0, s] + k.got2[p, 0, s].astype(F32) + k.got2[p, 1, s].astype(F32)
                    k.third[p] = k.kept[p, places(1 - p, 2)].astype(BF16)

        if finish:

            def last(stage):
                copies = []
                for p in (0, 1):
                    for n, by in enumerate((1, -1)):
                        if stage == 0:
                            some = pl.ds(0, cut) if n == 0 else pl.ds(cut, last_rows - cut)
                            src, dst = k.third_in.at[p, some], k.got3.at[p, some]
                        else:
                            src, dst = k.put4.at[p, n], k.got4.at[p, n]
                        copies.append(send(src, dst, k.last_send.at[stage, p, n], k.last_recv.at[stage, p, n], beside(1 - p, by)))
                return copies

            @when(0)
            def _():
                for copy in last(0):
                    copy.start()

            @when(3)
            def _():
                for copy in last(0):
                    copy.wait()
                for p in (0, 1):
                    ahead, behind = places(1 - p, 1), places(1 - p, -1)
                    k.put4[p, 0, :cut] = (k.kept_in[p, ahead, :cut] + k.got3[p, :cut].astype(F32)).astype(BF16)
                    k.put4[p, 0, cut:] = k.kept_in[p, ahead, cut:].astype(BF16)
                    k.put4[p, 1, :cut] = k.kept_in[p, behind, :cut].astype(BF16)
                    k.put4[p, 1, cut:] = (k.kept_in[p, behind, cut:] + k.got3[p, cut:].astype(F32)).astype(BF16)

            @when(4)
            def _():
                for copy in last(1):
                    copy.start()

            @when(9)
            def _():
                for copy in last(1):
                    copy.wait()
                for p in (0, 1):
                    mine = k.kept_in[p, places(1 - p, 0)]
                    both = mine + k.got4[p, 0].astype(F32) + k.got4[p, 1].astype(F32)
                    k.block[:, p * last_part : (p + 1) * last_part] = both.astype(BF16)

        if across is not None:
            sides = (pl.ds(0, wide_columns // 2), pl.ds(wide_columns // 2, wide_columns // 2))
            ways = ((near, wrap), (wrap, near))

            def swaps(stage):
                src = k.partial if stage == 0 else k.across_put
                return [
                    send(src.at[:, sides[p]], k.across_got.at[stage, :, sides[p]], k.across_send.at[stage, p], k.across_recv.at[stage, p], {"r": ways[p][stage](x)})
                    for p in (0, 1)
                ]

            @when(0)
            def _():
                for copy in swaps(0):
                    copy.start()

            @when(4)
            def _():
                for copy in swaps(0):
                    copy.wait()
                k.across_put[...] = (k.partial[...].astype(F32) + k.across_got[0].astype(F32)).astype(BF16)

            @when(5)
            def _():
                for copy in swaps(1):
                    copy.start()

            @when(10)
            def _():
                for copy in swaps(1):
                    copy.wait()
                k.total[...] = (k.across_put[...].astype(F32) + k.across_got[1].astype(F32)).astype(BF16)

        if product:

            def fetch(n):
                theirs = (n < tiles).astype(jnp.int32)
                which = theirs * (1 - c) + (1 - theirs) * c
                column = pl.multiple_of(which * half + (n - tiles * (1 - theirs)) * TILE, TILE)
                slot = lax.rem(n, 2)
                return pltpu.make_async_copy(k.streamed.at[:, pl.ds(column, TILE)], k.stream.at[slot], k.stream_sem.at[slot])

            def to_partner(n):
                return send(k.sent.at[n], k.came.at[n], k.pair_send.at[n], k.pair_recv.at[n], {"c": 1 - c})

            @when(0)
            def _():
                fetch(i).start()

        for step in sorted(events):

            @pl.when(i == step)
            def _(step=step):
                for f in events[step]:
                    f()

        if product:

            @pl.when(jnp.logical_and(i >= 1, i <= tiles))
            def _():
                to_partner(i - 1).start()

            @pl.when(i < 2 * tiles)
            def _():
                fetch(i).wait()

                @pl.when(i + 1 < 2 * tiles)
                def _():
                    fetch(i + 1).start()

                block = k.stream[lax.rem(i, 2)]
                if kind == "columns":
                    value = jnp.dot(k.resident[...], block, preferred_element_type=F32)
                else:
                    value = lax.dot_general(block, k.resident[...], (((0,), (0,)), ((), ())), preferred_element_type=F32)

                @pl.when(i < tiles)
                def _():
                    k.sent[i] = value.astype(BF16)

                @pl.when(i >= tiles)
                def _():
                    to_partner(i - tiles).wait()
                    both = value + k.came[i - tiles].astype(F32)
                    k.wide[...] = both
                    k.narrow[...] = both.astype(BF16)

    call = pl.pallas_call(
        kernel,
        grid=(steps,),
        out_shape=out_shapes,
        in_specs=in_specs,
        out_specs=out_specs,
        scratch_shapes=scratch,
        compiler_params=pltpu.CompilerParams(
            collective_id=number, has_side_effects=True, dimension_semantics=("arbitrary",), vmem_limit_bytes=62 * 1024 * 1024
        ),
        cost_estimate=pl.CostEstimate(flops=max(flops, 10**9), bytes_accessed=max(moved, 10**6), transcendentals=0),
        name=f"gradient{number}",
    )
    return dict(zip(names_out, call(*operands), strict=True))


def gathered_pair(number, one, two):
    rows, columns = one.shape[1:]
    halves = (pl.ds(0, columns // 2), pl.ds(columns // 2, columns // 2))
    every = pl.ds(0, SIDE)
    dma = pltpu.SemaphoreType.DMA

    def kernel(one_ref, two_ref, one_out, two_out, own_sem, ring_send, ring_recv, pair_send, pair_recv):
        q, c = lax.axis_index("q"), lax.axis_index("c")
        at = (q // SIDE, lax.rem(q, SIDE))
        ins, outs = (one_ref, two_ref), (one_out, two_out)

        def along(axis, by):
            return lax.rem(at[axis] + by + SIDE, SIDE)

        def beside(axis, by):
            return {"q": along(0, by) * SIDE + at[1] if axis == 0 else at[0] * SIDE + along(1, by)}

        def line(p, by, some=None):
            there = along(1 - p, by)
            some = pl.ds(0, columns) if some is None else some
            return outs[p].at[every, there, c, :, some] if p == 0 else outs[p].at[there, every, c, :, some]

        def single(p, by, some=None):
            there = along(p, by)
            some = pl.ds(0, columns) if some is None else some
            return outs[p].at[there, at[1], c, :, some] if p == 0 else outs[p].at[at[0], there, c, :, some]

        def send(src, dst, stage, p, n, to):
            return pltpu.make_async_remote_copy(
                src_ref=src, dst_ref=dst, send_sem=ring_send.at[stage, p, n], recv_sem=ring_recv.at[stage, p, n], device_id=to, device_id_type=MESH
            )

        def ring(stage):
            copies = []
            for p in (0, 1):
                for n, by in enumerate((1, -1)):
                    if stage == 0:
                        copies.append(send(ins[p].at[0], single(p, 0), stage, p, n, beside(p, by)))
                    elif stage == 1:
                        copies.append(send(single(p, -by, halves[n]), single(p, -by, halves[n]), stage, p, n, beside(p, by)))
                    elif stage == 2:
                        copies.append(send(line(p, 0), line(p, 0), stage, p, n, beside(1 - p, by)))
                    else:
                        copies.append(send(line(p, -by, halves[n]), line(p, -by, halves[n]), stage, p, n, beside(1 - p, by)))
            return copies

        def to_partner(by, n):
            return [
                pltpu.make_async_remote_copy(
                    src_ref=line(p, by),
                    dst_ref=line(p, by),
                    send_sem=pair_send.at[p, n],
                    recv_sem=pair_recv.at[p, n],
                    device_id={"c": 1 - c},
                    device_id_type=MESH,
                )
                for p in (0, 1)
            ]

        def start(copies):
            for copy in copies:
                copy.start()

        def wait(copies):
            for copy in copies:
                copy.wait()

        barrier = pltpu.get_barrier_semaphore()
        for peer in [{"c": 1 - c}] + [beside(axis, by) for axis in (0, 1) for by in (1, -1)]:
            pl.semaphore_signal(barrier, inc=1, device_id=peer, device_id_type=MESH)
        pl.semaphore_wait(barrier, 5)

        own = [pltpu.make_async_copy(ins[p].at[0], single(p, 0), own_sem.at[p]) for p in (0, 1)]
        start(ring(0))
        start(own)
        wait(ring(0))
        start(ring(1))
        wait(own)
        wait(ring(1))
        start(ring(2))
        start(to_partner(0, 0))
        wait(ring(2))
        start(ring(3))
        start(to_partner(1, 1))
        start(to_partner(-1, 2))
        wait(ring(3))
        start(to_partner(2, 3))
        for n, by in enumerate((0, 1, -1, 2)):
            wait(to_partner(by, n))

    shape = (SIDE, SIDE, 2, rows, columns)
    outs = pl.pallas_call(
        kernel,
        out_shape=[jax.ShapeDtypeStruct(shape, BF16)] * 2,
        in_specs=[pl.BlockSpec(memory_space=pltpu.VMEM)] * 2,
        out_specs=[pl.BlockSpec(memory_space=pl.ANY)] * 2,
        scratch_shapes=[dma((2,)), dma((4, 2, 2)), dma((4, 2, 2)), dma((2, 4)), dma((2, 4))],
        compiler_params=pltpu.CompilerParams(collective_id=number, has_side_effects=True),
        cost_estimate=pl.CostEstimate(flops=2 * 10**10, bytes_accessed=4 * 10**7, transcendentals=0),
        name="gathered_pair",
    )(one, two)
    return [out.reshape(SIDE * SIDE * 2 * rows, columns) for out in outs]


def plane_sum(number, value, chips):
    count = 2 * chips

    def kernel(value_ref, total_ref, got, send_sem, recv_sem):
        q, c = lax.axis_index("q"), lax.axis_index("c")
        me = 2 * q + c
        barrier = pltpu.get_barrier_semaphore()
        peers = [lax.rem(me + n, count) for n in range(1, count)]
        for peer in peers:
            pl.semaphore_signal(barrier, inc=1, device_id={"q": peer // 2, "c": lax.rem(peer, 2)}, device_id_type=MESH)
        pl.semaphore_wait(barrier, count - 1)
        copies = [
            pltpu.make_async_remote_copy(
                src_ref=value_ref,
                dst_ref=got.at[n],
                send_sem=send_sem.at[n],
                recv_sem=recv_sem.at[n],
                device_id={"q": peer // 2, "c": lax.rem(peer, 2)},
                device_id_type=MESH,
            )
            for n, peer in enumerate(peers)
        ]
        for copy in copies:
            copy.start()
        for copy in copies:
            copy.wait()
        total = value_ref[...]
        for n in range(count - 1):
            total = total + got[n]
        total_ref[...] = total

    return pl.pallas_call(
        kernel,
        out_shape=jax.ShapeDtypeStruct((8, 128), F32),
        in_specs=[pl.BlockSpec(memory_space=pltpu.VMEM)],
        out_specs=pl.BlockSpec(memory_space=pltpu.VMEM),
        scratch_shapes=[pltpu.VMEM((count - 1, 8, 128), F32), pltpu.SemaphoreType.DMA((count - 1,)), pltpu.SemaphoreType.DMA((count - 1,))],
        compiler_params=pltpu.CompilerParams(collective_id=number, has_side_effects=True),
        name="plane_sum",
    )(jnp.full((8, 128), value, F32))[0, 0]


def solution(mesh):
    reps, groups, shards = (mesh.shape[a] for a in ("rep", "r", "s"))
    chips = shards // 2
    fine = Mesh(mesh.devices.reshape(reps, groups, chips, 2), ("rep", "r", "q", "c"))
    from_half = [(2 * (s % chips) + s // chips, s) for s in range(shards)]

    def step(x, dy, *arrays):
        weights, m, v = (arrays[i : i + 3] for i in (0, 3, 6))
        layers = weights[0].shape[0]
        first = lax.axis_index("c") == 0

        def own(name, total):
            if name == 2:
                return lax.ppermute(total, ("q", "c"), from_half)
            low, high = jnp.split(total, 2, axis=0)
            keep, send = jnp.where(first, low, high), jnp.where(first, high, low)
            came = lax.ppermute(send, "c", SWAP)
            return jnp.concatenate([jnp.where(first, keep, came), jnp.where(first, came, keep)], 1)

        full = [
            [None if number == 0 and i < 2 else lax.all_gather(w[number], ("q", "c"), axis=0, tiled=True) for i, w in enumerate(weights)] for number in range(layers)
        ]
        full[0][:2] = gathered_pair(12, weights[0], weights[1])
        h, kept = x[0], []
        for number in range(layers):
            w = full[number]
            a, back = jax.vjp(normed, h)
            gate = jnp.dot(a, w[0], preferred_element_type=F32)
            up = jnp.dot(a, w[1], preferred_element_type=F32)
            act = (jax.nn.silu(gate) * up).astype(BF16)
            kept.append((a, back, gate, up, act))
            if number < layers - 1:
                h = h + matmul(act, w[2])

        totals = [[None] * layers for _ in range(3)]
        state = {"number": 0, "scatter": None, "finish": None, "across": None}

        def run(product=None, name=None, number=None):
            one, two, three = (state[which] for which in ("scatter", "finish", "across"))
            given = gradient_call(state["number"], product, one and one[1], two and two[1], three and three[1])
            state["number"] += 1
            state["scatter"] = None
            if three is not None:
                totals[three[0][0]][three[0][1]] = given["total"]
            state["across"] = two and (two[0], given["block"])
            state["finish"] = one and (one[0], (given["kept"], given["third"]))
            if product is not None:
                shape = (SIDE, SIDE, given["wide"].shape[0] // chips, given["wide"].shape[1])
                state["scatter"] = ((name, number), (given["wide"].reshape(shape), given["narrow"].reshape(shape)))

        by_h = dy[0]
        for number in reversed(range(layers)):
            w = full[number]
            a, back, gate, up, act = kept[number]
            across_tokens = a.T
            run(("rows", by_h, act), 2, number)
            by_act = lax.dot_general(by_h, w[2], (((1,), (1,)), ((), ())), preferred_element_type=F32).astype(BF16).astype(F32)
            on = jax.nn.sigmoid(gate)
            by_up = (by_act * (gate * on)).astype(BF16)
            by_gate = (by_act * up * (on * (1.0 + gate * (1.0 - on)))).astype(BF16)
            run(("columns", across_tokens, by_gate), 0, number)
            run(("columns", across_tokens, by_up), 1, number)
            if number > 0:
                by_a = [
                    lax.dot_general(by, w[i], (((1,), (1,)), ((), ())), preferred_element_type=F32).astype(BF16) for i, by in ((0, by_gate), (1, by_up))
                ]
                by_h = by_h + back(by_a[0] + by_a[1])[0]
        for _ in range(3):
            run()

        squares = sum(jnp.sum(t.astype(F32) ** 2) for one in totals for t in one)
        squares = plane_sum(state["number"], squares, chips)
        gradients = [jnp.stack([own(name, t) for t in one]).astype(F32) for name, one in enumerate(totals)]
        count = shards * sum(g.size for g in gradients)
        factor = jnp.minimum(1.0, 0.5 * lax.rsqrt(squares / count + 1e-30))
        new = [adamw(w.astype(F32), m, v, g * factor) for w, m, v, g in zip(weights, m, v, gradients, strict=True)]
        return tuple(one[which] for which in range(3) for one in new)

    states, cut = P(("rep", "r", "q", "c"), None, None), P(None, ("q", "c"), None)
    return jax.shard_map(
        step,
        mesh=fine,
        in_specs=(states, states) + (cut,) * 9,
        out_specs=(P("rep", ("q", "c"), None),) * 9,
        check_vma=False,
    )
```
